32 devices in a mesh: zero: 8 (over z, x), tp: 4 (over y, core).
Axes of the slice: x: 2, y: 2, z: 4, core: 2. Of those that a mesh axis runs over, the one named last changes fastest.
Arguments:
- train_gate: float32 [2048, 8192], P('zero', 'tp'), may hold values from -0.1875 to 0.1875
- slow_gate: float32 [2048, 8192], P('zero', 'tp'), may hold values from -0.125 to 0.125
- train_up: float32 [2048, 8192], P('zero', 'tp'), may hold values from -0.1875 to 0.1875
- slow_up: float32 [2048, 8192], P('zero', 'tp'), may hold values from -0.125 to 0.125
- norm_gain: float32 [2048], P('zero'), may hold values from 0.25 to 1.75
Outputs:
- serving_gate: bfloat16 [2048, 8192], P(None, 'tp')
- serving_up: bfloat16 [2048, 8192], P(None, 'tp')
- scale_gate: float32 [8192], P('tp')
- scale_up: float32 [8192], P('tp')
The draws below stay inside these ranges and needn't reach their ends.
All inputs are finite; a program needn't handle non-finite values.
Results may differ from the reference program's by a relative error of at most 0.0004.
Values may be sent and summed in bfloat16 or wider, within the bound.
No kernel may reach another device: no remote copies, remote signals or barrier semaphores. Data moves between devices by JAX's collectives and lax.ppermute only.
A program may use at most 128 MiB of HBM per device.

```python
import jax
import jax.numpy as jnp
from jax import lax

D_MODEL = 2048
D_INNER = 8192


def spiked(drawn, key, source, target, shards_of, factor):
    def block_of(axis_at):
        return (jnp.arange(drawn.shape[axis_at]) // (drawn.shape[axis_at] // shards_of)).reshape((-1,) + (1,) * (drawn.ndim - 1 - axis_at))

    near = jax.random.permutation(key, shards_of)[block_of(target)]
    second = (block_of(target) + shards_of // 2) % shards_of
    return jnp.where((block_of(source) == near) | (block_of(source) == second), factor * drawn, drawn)


def block_scale(own_key, dims, split, least, largest):
    gain, own = 1.0, jax.random.fold_in(own_key, 6)
    for dim, parts in split:
        draws = jnp.exp(jax.random.uniform(jax.random.fold_in(own, dim), (parts,), jnp.float32, least / len(split), largest / len(split)))
        gain = gain * jnp.repeat(draws, dims[dim] // parts).reshape([-1 if axis == dim else 1 for axis in range(len(dims))])
    return gain


def gaussian(rng, shape, scale, most, cuts=(), held_as=jnp.bfloat16):
    factor_of = block_scale(rng, shape, cuts, -0.22, 0.18) if cuts else 1.0
    array = jax.random.normal(rng, shape, jnp.float32) * scale * factor_of
    return jnp.minimum(jnp.maximum(array, -most), most).astype(held_as)


def gaussian_with(stream_key, dims, width, bound, pieces, heavy, held_as=jnp.bfloat16):
    array = width * jax.random.normal(stream_key, dims, jnp.float32)
    if pieces:
        array = array * block_scale(stream_key, dims, pieces, -0.22, 0.18)
    return jnp.clip(spiked(array, jax.random.fold_in(stream_key, 3), *heavy), -bound, bound).astype(held_as)


def setup_inputs(seed: int = 0) -> dict:
    arg_keys = jax.random.split(jax.random.key(seed), 6)
    train_gate = gaussian_with(arg_keys[0], (D_MODEL, D_INNER), D_MODEL ** -0.5, 0.1875, ((0, 8), (1, 4)), (0, 1, 8, 2.0), jnp.float32)
    slow_gate = gaussian(arg_keys[1], (D_MODEL, D_INNER), D_MODEL ** -0.5, 0.125, ((0, 8), (1, 4)), jnp.float32)
    train_up = gaussian_with(arg_keys[2], (D_MODEL, D_INNER), D_MODEL ** -0.5, 0.1875, ((0, 8), (1, 4)), (0, 1, 8, 2.0), jnp.float32)
    slow_up = gaussian(arg_keys[3], (D_MODEL, D_INNER), D_MODEL ** -0.5, 0.125, ((0, 8), (1, 4)), jnp.float32)
    norm_gain = jnp.clip(1.0 + 0.15 * jax.random.normal(arg_keys[4], (D_MODEL,), jnp.float32), 0.25, 1.75)
    return {"train_gate": train_gate, "slow_gate": slow_gate, "train_up": train_up, "slow_up": slow_up, "norm_gain": norm_gain}


keep_rate = 0.75

def reference(train_gate, slow_gate, train_up, slow_up, norm_gain):
    whole_gate = keep_rate * slow_gate + (1.0 - keep_rate) * train_gate
    whole_up = keep_rate * slow_up + (1.0 - keep_rate) * train_up
    whole_gained_gate = whole_gate * norm_gain[:, None]
    whole_gained_up = whole_up * norm_gain[:, None]
    scale_gate = jnp.sqrt(lax.optimization_barrier(jnp.sum(whole_gained_gate * whole_gained_gate, axis=0)))
    serving_gate = (whole_gained_gate / scale_gate).astype(jnp.bfloat16)
    scale_up = jnp.sqrt(lax.optimization_barrier(jnp.sum(whole_gained_up * whole_gained_up, axis=0)))
    serving_up = (whole_gained_up / scale_up).astype(jnp.bfloat16)
    return (serving_gate, serving_up, scale_gate, scale_up)
```

```python
import jax
import jax.numpy as jnp
from jax import lax
from jax.sharding import PartitionSpec as P

keep_rate = 0.75


def all_sum(value, size):
    if size & (size - 1):
        return lax.psum(value, "zero")
    stride = 1
    while stride < size:
        pairs = [(i, i ^ stride) for i in range(size)]
        value = value + lax.ppermute(value, "zero", pairs)
        stride *= 2
    return value


def solution(mesh):
    size = mesh.shape["zero"]
    inner = 2 if size % 2 == 0 else 1
    outer = size // inner
    ring = [(i, (i + inner) % size) for i in range(size)]
    swap = [(i, i ^ 1) for i in range(size)]

    def place(out, piece, owner, start, rows):
        return lax.dynamic_update_slice(out, piece, (owner * rows + start, 0))

    def swapped(piece):
        return lax.ppermute(piece, "zero", swap) if inner == 2 else None

    def body(train_gate, slow_gate, train_up, slow_up, norm_gain):
        rows, columns = train_gate.shape
        me = lax.axis_index("zero")
        gained_gate = (keep_rate * slow_gate + (1.0 - keep_rate) * train_gate) * norm_gain[:, None]
        gained_up = (keep_rate * slow_up + (1.0 - keep_rate) * train_up) * norm_gain[:, None]
        sums = jnp.stack([jnp.sum(gained_gate * gained_gate, axis=0), jnp.sum(gained_up * gained_up, axis=0)])
        scales = jnp.sqrt(all_sum(sums, size))
        scale_gate, scale_up = scales[0], scales[1]
        narrow_gate = (gained_gate / scale_gate).astype(jnp.bfloat16)
        narrow_up = (gained_up / scale_up).astype(jnp.bfloat16)

        if outer > 8:
            out_gate = lax.all_gather(narrow_gate, "zero", axis=0, tiled=True)
            out_up = lax.all_gather(narrow_up, "zero", axis=0, tiled=True)
            return (out_gate, out_up, scale_gate, scale_up)

        first = max(16, rows * 5 // 16 // 16 * 16) if inner == 2 and rows >= 32 else 0
        cut = rows - first
        out_gate = jnp.zeros((size * rows, columns), jnp.bfloat16)
        out_up = jnp.zeros((size * rows, columns), jnp.bfloat16)

        def put(which, piece, owner, start):
            nonlocal out_gate, out_up
            if which == 0:
                out_gate = place(out_gate, piece, owner, start, rows)
            else:
                out_up = place(out_up, piece, owner, start, rows)

        held = [(0, 0, narrow_gate), (1, 0, narrow_up[:cut])]
        pair = None
        if first:
            own = narrow_up[cut:]
            other = swapped(own)
            put(1, own, me, cut)
            put(1, other, me ^ 1, cut)
            pair = [own, other]
        for step in range(outer):
            owner = (me + size - inner * step) % size
            coming = []
            for which, start, piece in held:
                if step < outer - 1:
                    coming.append((which, start, lax.ppermute(piece, "zero", ring)))
                if inner == 2:
                    put(which, swapped(piece), owner ^ 1, start)
                put(which, piece, owner, start)
            held = coming
            if pair is not None and step < outer - 1:
                pair = [lax.ppermute(piece, "zero", ring) for piece in pair]
                source = (me + size - inner * (step + 1)) % size
                put(1, pair[0], source, cut)
                put(1, pair[1], source ^ 1, cut)
        return (out_gate, out_up, scale_gate, scale_up)

    in_specs = (P("zero", "tp"), P("zero", "tp"), P("zero", "tp"), P("zero", "tp"), P("zero"))
    out_specs = (P(None, "tp"), P(None, "tp"), P("tp"), P("tp"))
    return jax.shard_map(body, mesh=mesh, in_specs=in_specs, out_specs=out_specs, check_vma=False)
```

```python
import jax
import jax.numpy as jnp
from jax import lax
from jax.experimental import pallas as pl
from jax.experimental.pallas import tpu as pltpu
from jax.sharding import PartitionSpec as P

keep_rate = 0.75
in_flight = 2


def all_sum(value, size):
    if size & (size - 1):
        return lax.psum(value, "zero")
    stride = 1
    while stride < size:
        pairs = [(i, i ^ stride) for i in range(size)]
        value = value + lax.ppermute(value, "zero", pairs)
        stride *= 2
    return value


def unwritten(shape, dtype):
    return pl.pallas_call(
        lambda out_ref: None,
        out_shape=jax.ShapeDtypeStruct(shape, dtype),
        out_specs=pl.BlockSpec(memory_space=pltpu.HBM),
    )()


def plan(outer, rows, cut):
    first = rows - cut
    z, x = [], [(("x", "g", 0), ("z", "g", 0), rows)]
    if first:
        x.append((("x", "v", 0), ("z", "v", 0), first))
    for step in range(1, outer):
        z.append((("z", "g", step), ("z", "g", step - 1), rows))
        if first and step >= 2:
            z.append((("z", "v", step - 1), ("z", "v", step - 2), 2 * first))
        z.append((("z", "u", step), ("z", "u", step - 1), cut))
        if step == 1:
            x.append((("x", "g", 1), ("z", "g", 1), rows))
            x.append((("x", "u", 0), ("z", "u", 0), cut))
        else:
            x.append((("x", "g", step), ("z", "g", step), rows))
        x.append((("x", "u", step), ("z", "u", step), cut))
    if outer == 1:
        x.append((("x", "u", 0), ("z", "u", 0), cut))
    elif first:
        z.append((("z", "v", outer - 1), ("z", "v", outer - 2), 2 * first))
    ended = {("z", kind, 0): 0 for kind in "guv"}
    issued, todo = [], {"z": list(z), "x": list(x)}
    done = {"z": [], "x": []}
    while todo["z"] or todo["x"]:
        options = []
        for link in "zx":
            if todo[link]:
                name, source, length = todo[link][0]
                if source in ended and not (name == ("z", "v", 1) and ("x", "v", 0) not in ended):
                    ready = ended[source]
                    if name == ("z", "v", 1):
                        ready = max(ready, ended[("x", "v", 0)])
                    if len(done[link]) >= in_flight:
                        ready = max(ready, done[link][-in_flight][0])
                    begin = max(ready, done[link][-1][0] if done[link] else 0)
                    options.append((ready, link, begin + length, name, source))
        ready, link, end, name, source = min(options)
        todo[link].pop(0)
        ended[name] = end
        before = [(e, n) for l in "zx" for e, n in done[l] if e <= ready]
        tied = [max(before)[1]] if before else []
        if len(done[link]) >= in_flight:
            tied.append(done[link][-in_flight][1])
        done[link].append((end, name))
        issued.append((name, source, [t for t in dict.fromkeys(tied) if t != source]))
    return issued


def solution(mesh):
    size = mesh.shape["zero"]
    inner = 2 if size % 2 == 0 else 1
    outer = size // inner
    ring = [(i, (i + inner) % size) for i in range(size)]
    swap = [(i, i ^ 1) for i in range(size)]

    def body(train_gate, slow_gate, train_up, slow_up, norm_gain):
        rows, columns = train_gate.shape
        me = lax.axis_index("zero")
        gained_gate = (keep_rate * slow_gate + (1.0 - keep_rate) * train_gate) * norm_gain[:, None]
        gained_up = (keep_rate * slow_up + (1.0 - keep_rate) * train_up) * norm_gain[:, None]
        sums = jnp.stack([jnp.sum(gained_gate * gained_gate, axis=0), jnp.sum(gained_up * gained_up, axis=0)])
        scales = jnp.sqrt(all_sum(sums, size))
        scale_gate, scale_up = scales[0], scales[1]
        narrow_gate = (gained_gate / scale_gate).astype(jnp.bfloat16)
        if inner == 1 or outer > 8:
            narrow_up = (gained_up / scale_up).astype(jnp.bfloat16)
            out_gate = lax.all_gather(narrow_gate, "zero", axis=0, tiled=True)
            out_up = lax.all_gather(narrow_up, "zero", axis=0, tiled=True)
            return (out_gate, out_up, scale_gate, scale_up)

        narrow_gate, late_scale = lax.optimization_barrier((narrow_gate, scale_up))
        first = max(16, rows * 5 // 16 // 16 * 16) if rows >= 32 else 0
        cut = rows - first

        outs = [unwritten((size * rows, columns), jnp.bfloat16) for _ in range(2)]

        def put(which, piece, owner, start):
            outs[which] = lax.dynamic_update_slice(outs[which], piece, (owner * rows + start, 0))

        held = {("z", "g", 0): (narrow_gate,)}
        held["z", "u", 0] = ((gained_up[:cut] / late_scale).astype(jnp.bfloat16),)
        held["z", "v", 0] = ((gained_up[cut:] / late_scale).astype(jnp.bfloat16),)
        put(0, narrow_gate, me, 0)
        put(1, held["z", "u", 0][0], me, 0)
        if first:
            put(1, held["z", "v", 0][0], me, cut)
        for name, source, tied in plan(outer, rows, cut):
            link, kind, step = name
            pieces = held[source]
            if name == ("z", "v", 1):
                pieces = pieces + held["x", "v", 0]
            if tied:
                pieces = lax.optimization_barrier((pieces, [held[t] for t in tied]))[0]
            held[name] = tuple(lax.ppermute(p, "zero", ring if link == "z" else swap) for p in pieces)
            owner = (me + size - inner * step) % size
            for at, piece in enumerate(held[name]):
                turned = at == 1 or link == "x"
                which, start = (0, 0) if kind == "g" else (1, 0 if kind == "u" else cut)
                put(which, piece, owner ^ 1 if turned else owner, start)
        return (outs[0], outs[1], scale_gate, scale_up)

    in_specs = (P("zero", "tp"), P("zero", "tp"), P("zero", "tp"), P("zero", "tp"), P("zero"))
    out_specs = (P(None, "tp"), P(None, "tp"), P("tp"), P("tp"))
    return jax.shard_map(body, mesh=mesh, in_specs=in_specs, out_specs=out_specs, check_vma=False)
```

```python
import jax
import jax.numpy as jnp
from jax import lax
from jax.experimental import pallas as pl
from jax.experimental.pallas import tpu as pltpu
from jax.sharding import PartitionSpec as P

keep_rate = 0.75
in_flight = 2


def all_sum(value, size):
    if size & (size - 1):
        return lax.psum(value, "zero")

    def from_partner(stride):
        return lax.ppermute(value, "zero", [(i, i ^ stride) for i in range(size)])

    left = size
    while left > 1:
        stride = size // left
        if left % 4 == 0:
            near, far, both = (from_partner(stride * k) for k in (1, 2, 3))
            value = (value + near) + (far + both)
            left //= 4
        else:
            value = value + from_partner(stride)
            left //= 2
    return value


def unwritten(shape, dtype):
    return pl.pallas_call(
        lambda out_ref: None,
        out_shape=jax.ShapeDtypeStruct(shape, dtype),
        out_specs=pl.BlockSpec(memory_space=pltpu.HBM),
    )()


def plan(outer, rows, cut):
    first = rows - cut
    z, x = [], [(("x", "g", 0), ("z", "g", 0), rows)]
    if first:
        x.append((("x", "v", 0), ("z", "v", 0), first))
    for step in range(1, outer):
        z.append((("z", "g", step), ("z", "g", step - 1), rows))
        if first and step >= 2:
            z.append((("z", "v", step - 1), ("z", "v", step - 2), 2 * first))
        z.append((("z", "u", step), ("z", "u", step - 1), cut))
        if step == 1:
            x.append((("x", "g", 1), ("z", "g", 1), rows))
            x.append((("x", "u", 0), ("z", "u", 0), cut))
        else:
            x.append((("x", "g", step), ("z", "g", step), rows))
        x.append((("x", "u", step), ("z", "u", step), cut))
    if outer == 1:
        x.append((("x", "u", 0), ("z", "u", 0), cut))
    elif first:
        z.append((("z", "v", outer - 1), ("z", "v", outer - 2), 2 * first))
    ended = {("z", kind, 0): 0 for kind in "guv"}
    issued, todo = [], {"z": list(z), "x": list(x)}
    done = {"z": [], "x": []}
    while todo["z"] or todo["x"]:
        options = []
        for link in "zx":
            if todo[link]:
                name, source, length = todo[link][0]
                if source in ended and not (name == ("z", "v", 1) and ("x", "v", 0) not in ended):
                    ready = ended[source]
                    if name == ("z", "v", 1):
                        ready = max(ready, ended[("x", "v", 0)])
                    if len(done[link]) >= in_flight:
                        ready = max(ready, done[link][-in_flight][0])
                    begin = max(ready, done[link][-1][0] if done[link] else 0)
                    options.append((ready, link, begin + length, name, source))
        ready, link, end, name, source = min(options)
        todo[link].pop(0)
        ended[name] = end
        before = [(e, n) for l in "zx" for e, n in done[l] if e <= ready]
        tied = [max(before)[1]] if before else []
        if len(done[link]) >= in_flight:
            tied.append(done[link][-in_flight][1])
        done[link].append((end, name))
        issued.append((name, source, [t for t in dict.fromkeys(tied) if t != source]))
    return issued


def solution(mesh):
    size = mesh.shape["zero"]
    inner = 2 if size % 2 == 0 else 1
    outer = size // inner
    ring = [(i, (i + inner) % size) for i in range(size)]
    swap = [(i, i ^ 1) for i in range(size)]

    def body(train_gate, slow_gate, train_up, slow_up, norm_gain):
        rows, columns = train_gate.shape
        me = lax.axis_index("zero")
        gained_gate = (keep_rate * slow_gate + (1.0 - keep_rate) * train_gate) * norm_gain[:, None]
        gained_up = (keep_rate * slow_up + (1.0 - keep_rate) * train_up) * norm_gain[:, None]
        sums = jnp.stack([jnp.sum(gained_gate * gained_gate, axis=0), jnp.sum(gained_up * gained_up, axis=0)])
        scales = jnp.sqrt(all_sum(sums, size))
        scale_gate, scale_up = scales[0], scales[1]
        narrow_gate = (gained_gate / scale_gate).astype(jnp.bfloat16)
        if inner == 1 or outer > 8:
            narrow_up = (gained_up / scale_up).astype(jnp.bfloat16)
            out_gate = lax.all_gather(narrow_gate, "zero", axis=0, tiled=True)
            out_up = lax.all_gather(narrow_up, "zero", axis=0, tiled=True)
            return (out_gate, out_up, scale_gate, scale_up)

        narrow_gate, late_scale = lax.optimization_barrier((narrow_gate, scale_up))
        first = max(16, rows * 5 // 16 // 16 * 16) if rows >= 32 else 0
        cut = rows - first

        outs = [unwritten((size * rows, columns), jnp.bfloat16) for _ in range(2)]

        def put(which, piece, owner, start):
            outs[which] = lax.dynamic_update_slice(outs[which], piece, (owner * rows + start, 0))

        held = {("z", "g", 0): (narrow_gate,)}
        held["z", "u", 0] = ((gained_up[:cut] / late_scale).astype(jnp.bfloat16),)
        held["z", "v", 0] = ((gained_up[cut:] / late_scale).astype(jnp.bfloat16),)
        put(0, narrow_gate, me, 0)
        put(1, held["z", "u", 0][0], me, 0)
        if first:
            put(1, held["z", "v", 0][0], me, cut)
        for name, source, tied in plan(outer, rows, cut):
            link, kind, step = name
            pieces = held[source]
            if name == ("z", "v", 1):
                pieces = pieces + held["x", "v", 0]
            if tied:
                pieces = lax.optimization_barrier((pieces, [held[t] for t in tied]))[0]
            held[name] = tuple(lax.ppermute(p, "zero", ring if link == "z" else swap) for p in pieces)
            owner = (me + size - inner * step) % size
            for at, piece in enumerate(held[name]):
                turned = at == 1 or link == "x"
                which, start = (0, 0) if kind == "g" else (1, 0 if kind == "u" else cut)
                put(which, piece, owner ^ 1 if turned else owner, start)
        return (outs[0], outs[1], scale_gate, scale_up)

    in_specs = (P("zero", "tp"), P("zero", "tp"), P("zero", "tp"), P("zero", "tp"), P("zero"))
    out_specs = (P(None, "tp"), P(None, "tp"), P("tp"), P("tp"))
    return jax.shard_map(body, mesh=mesh, in_specs=in_specs, out_specs=out_specs, check_vma=False)
```
